32 devices in a mesh: bank: 4 (over x, core), lane: 8 (over z, y).
Axes of the slice: x: 2, y: 2, z: 4, core: 2. Of those that a mesh axis runs over, the one named last changes fastest.
Arguments:
- amplitudes: float32 [2, 256, 128, 128], P(None, ('bank', 'lane')), may hold values from -6 to 6
- energies: float32 [256, 128, 128], P(('bank', 'lane')), may hold values from -2 to 2
- diagonal_angles: float32 [2, 128], replicated, may hold values from 0.3 to 1.2
Outputs:
- final_parts: float32 [2, 256, 128, 128], P(None, ('bank', 'lane'))
- marginal: float32 [64, 128, 128], P('lane', 'bank')
The draws below stay inside these ranges and needn't reach their ends.
All inputs are finite; a program needn't handle non-finite values.
Results may differ from the reference program's by a relative error of at most 0.0003.
Values sent between devices are 32-bit elements; how exact they have to be, the bound alone decides.
A program may use at most 64 MiB of HBM per device.

```python
import jax
import jax.numpy as jnp
from jax import lax

BLOCKS_DEV = 8
ROWS = 128
LANES = 128
BLOCKS = 256
LAYERS = 2
N_BANK = 4
N_LANE = 8


def block_scale(stream_key, dims, pieces, smallest, high):
    loudness, own = 1.0, jax.random.fold_in(stream_key, 6)
    for position, blocks in pieces:
        heights = jnp.exp(jax.random.uniform(jax.random.fold_in(own, position), (blocks,), jnp.float32, smallest / len(pieces), high / len(pieces)))
        loudness = loudness * jnp.repeat(heights, dims[position] // blocks).reshape([-1 if axis == position else 1 for axis in range(len(dims))])
    return loudness


def normal_values(key, shape, width, most, shards=(), held_as=jnp.bfloat16):
    drawn = width * jax.random.normal(key, shape, jnp.float32)
    if shards:
        drawn = drawn * block_scale(key, shape, shards, -0.22, 0.18)
    return jnp.clip(drawn, -most, most).astype(held_as)


def setup_inputs(seed: int = 0) -> dict:
    splits = jax.random.split(jax.random.key(seed), 4)
    return {
        "amplitudes": normal_values(splits[0], (2, BLOCKS, ROWS, LANES), 1.0, 6.0, ((1, 32),), jnp.float32),
        "energies": jnp.clip(jax.random.uniform(splits[1], (BLOCKS, ROWS, LANES), jnp.float32, -2.0, 2.0) * block_scale(splits[1], (BLOCKS, ROWS, LANES), ((0, 32),), -0.4, 0.0), -2.0, 2.0),
        "diagonal_angles": jnp.clip(jax.random.uniform(splits[2], (LAYERS, LANES), jnp.float32, 0.3, 1.2), 0.3, 1.2),
    }


def count_bits(values, count):
    places = jnp.arange(count.bit_length() - 1, dtype=jnp.int32)
    return jnp.sum((values[..., None] >> places) & 1, axis=-1)


def walsh_table(count):
    rank = jnp.arange(count, dtype=jnp.int32)
    parity = count_bits(rank[:, None] & rank[None, :], count) % 2
    real_part = jnp.where(parity == 1, -1.0, 1.0).astype(jnp.float32) * (count ** -0.5)
    return real_part


def apply_along(values, dim):
    real_part = walsh_table(values.shape[dim])
    def times(table):
        moved = jnp.tensordot(values, table, axes=([dim], [0]), precision=lax.Precision.HIGHEST)
        return jnp.moveaxis(moved, -1, dim)
    return times(real_part)


def diagonal_step(values, levels, angle):
    turn = angle * levels
    return jnp.stack([values[0] * jnp.cos(turn) + values[1] * jnp.sin(turn), values[1] * jnp.cos(turn) - values[0] * jnp.sin(turn)])


def reference(amplitudes, energies, diagonal_angles):
    values = amplitudes
    for layer in range(LAYERS):
        values = diagonal_step(values, energies, diagonal_angles[layer])
        values = apply_along(values, 3)
        values = apply_along(values, 2)
        parts = values.reshape(2, N_BANK, N_LANE, BLOCKS_DEV, ROWS, LANES)
        parts = apply_along(parts, 1)
        parts = apply_along(parts, 2)
        parts = apply_along(parts, 3)
        values = parts.reshape(values.shape)
    chance = values[0] * values[0] + values[1] * values[1]
    marginal = jnp.mean(chance.reshape(N_BANK, -1, ROWS, LANES), axis=0)
    return values, marginal
```

```python
import functools

import jax
import jax.numpy as jnp
import numpy as np
from jax import lax
from jax.experimental import pallas as pl
from jax.experimental.pallas import tpu as pltpu
from jax.sharding import PartitionSpec as P

MESH = pl.DeviceIdType.MESH
TABLE = 256
SUB = 8
CHUNKS = 4


def walsh_table():
    rank = np.arange(TABLE)
    both = rank[:, None] & rank[None, :]
    parity = sum((both >> place) & 1 for place in range(8)) % 2
    return jnp.asarray(np.where(parity == 1, -1.0, 1.0) / 16.0, jnp.bfloat16)


def cos_sin(turn):
    half = turn * 0.5
    x = half * half
    s = -1.0 / 39916800.0
    for term in (1.0 / 362880.0, -1.0 / 5040.0, 1.0 / 120.0, -1.0 / 6.0, 1.0):
        s = s * x + term
    s = s * half
    c = 1.0 / 479001600.0
    for term in (-1.0 / 3628800.0, 1.0 / 40320.0, -1.0 / 720.0, 1.0 / 24.0, -0.5, 1.0):
        c = c * x + term
    return 1.0 - 2.0 * (s * s), 2.0 * (s * c)


def split(values):
    high = values.astype(jnp.bfloat16)
    return high, (values - high.astype(jnp.float32)).astype(jnp.bfloat16)


def mix(items):
    items, step = list(items), 1
    while step < len(items):
        for low in range(len(items)):
            if not low & step:
                u, v = items[low], items[low + step]
                items[low], items[low + step] = u + v, u - v
        step *= 2
    return items


def dot(a, b):
    return jnp.dot(a, b, preferred_element_type=jnp.float32)


def mix_lanes(values, table):
    high, low = split(values)
    return dot(jnp.concatenate([high, low], axis=1), table[:, :128])


def kernel(
    n_bank, n_lane, chunks,
    a_ref, e_ref, angle_ref, table_ref,
    out_ref, marginal_ref,
    held, sent1, got1, sent2, got2, levels, cosine, sine, chance, chances,
    e_send, e_recv, send1, recv1, send2, recv2, m_send, m_recv,
):
    devices = n_bank * n_lane
    _, blocks, rows, lanes = a_ref.shape
    group = blocks * rows // devices
    piece = group // chunks
    groups = rows // group
    tiles = piece // SUB
    bank, lane = lax.axis_index("bank"), lax.axis_index("lane")
    me = bank * n_lane + lane

    def place(device):
        return (device // n_lane, device % n_lane)

    barrier = pltpu.get_barrier_semaphore()

    def greet(step, _):
        pl.semaphore_signal(
            barrier, inc=1, device_id=place((me + step) % devices), device_id_type=MESH
        )
        return 0

    lax.fori_loop(1, devices, greet, 0)
    pl.semaphore_wait(barrier, devices - 1)

    def swap(src, dst, send_sem, recv_sem):
        def one(step, _):
            other = (me + step) % devices
            pltpu.make_async_remote_copy(
                src_ref=src.at[other], dst_ref=dst.at[me],
                send_sem=send_sem, recv_sem=recv_sem,
                device_id=place(other), device_id_type=MESH,
            ).start()
            return 0

        lax.fori_loop(1, devices, one, 0)

    def arrive(buffer, sem):
        most = buffer.at[pl.ds(0, devices - 1)]
        pltpu.make_async_copy(most, most, sem).wait()

    swap(e_ref, levels, e_send, e_recv)
    levels[me] = e_ref[me]

    table = table_ref[...]

    def block_step(b, _):
        first = b * groups
        level = e_ref[pl.ds(first, groups)].reshape(rows, lanes)
        c, s = cos_sin(level * angle_ref[0:1, :])
        re, im = a_ref[0, b], a_ref[1, b]
        turned = jnp.concatenate([re * c + im * s, im * c - re * s], axis=0)
        along = mix_lanes(turned, table)
        high, low = split(jnp.concatenate([along[:rows], along[rows:]], axis=1))
        mixed = dot(table[:128, :], jnp.concatenate([high, low], axis=0))
        held[b, 0] = mixed[:, :lanes]
        held[b, 1] = mixed[:, lanes:]
        return 0

    lax.fori_loop(0, blocks, block_step, 0)

    for chunk in range(chunks):
        def spread(g, _, chunk=chunk):
            start = pl.multiple_of(g * group + chunk * piece, SUB)
            for part in range(2):
                mixed = mix([held[b, part, pl.ds(start, piece), :] for b in range(blocks)])
                for b in range(blocks):
                    sent1[chunk, b * groups + g, part] = mixed[b]
            return 0

        lax.fori_loop(0, groups, spread, 0)
        swap(sent1.at[chunk], got1.at[chunk], send1.at[chunk], recv1.at[chunk])
        got1[chunk, me] = sent1[chunk, me]

    arrive(levels, e_recv)

    def phases(d, _):
        c, s = cos_sin(levels[d] * angle_ref[1:2, :])
        cosine[d] = c
        sine[d] = s
        return 0

    lax.fori_loop(0, devices, phases, 0)

    wide = TABLE // SUB
    for chunk in range(chunks):
        arrive(got1.at[chunk], recv1.at[chunk])
        for tile in range(tiles):
            here = pl.ds(tile * SUB, SUB)
            there = pl.ds(chunk * piece + tile * SUB, SUB)
            re = mix([got1[chunk, d, 0, here, :] for d in range(devices)])
            im = mix([got1[chunk, d, 1, here, :] for d in range(devices)])
            done = []
            for start in range(0, devices, wide):
                span = range(start, start + wide)
                r, i = [], []
                for d in span:
                    c, s = cosine[d, there, :], sine[d, there, :]
                    r.append(re[d] * c + im[d] * s)
                    i.append(im[d] * c - re[d] * s)
                along = mix_lanes(jnp.concatenate(r + i, axis=0), table)
                pair = jnp.concatenate([along[:TABLE], along[TABLE:]], axis=1)
                high, low = split(pair)
                done.append(dot(table, high) + dot(table, low))
            done = mix(done)
            for d in range(devices):
                at = d % wide * SUB
                tile_of = done[d // wide][at : at + SUB]
                sent2[chunk, d, 0, here, :] = tile_of[:, :lanes]
                sent2[chunk, d, 1, here, :] = tile_of[:, lanes:]
        swap(sent2.at[chunk], got2.at[chunk], send2.at[chunk], recv2.at[chunk])
        got2[chunk, me] = sent2[chunk, me]

    for chunk in range(chunks):
        arrive(got2.at[chunk], recv2.at[chunk])
        for tile in range(tiles):
            here = pl.ds(tile * SUB, SUB)
            for part in range(2):
                mixed = mix([got2[chunk, d, part, here, :] for d in range(devices)])
                for d in range(devices):
                    got2[chunk, d, part, here, :] = mixed[d]

    scale = float(TABLE * TABLE) / (devices * blocks * rows * lanes)
    strip = rows // n_bank

    def finish(d, _):
        b, row = d // groups, d % groups * group
        both = []
        for part in range(2):
            both.append(mix([
                got2[chunk, d, part, tile * SUB : (tile + 1) * SUB, :]
                for chunk in range(chunks) for tile in range(tiles)
            ]))
        for place_, (r, i) in enumerate(zip(*both)):
            r, i = r * scale, i * scale
            at = row + place_ * SUB
            out_ref[0, b, pl.ds(pl.multiple_of(at, SUB), SUB), :] = r
            out_ref[1, b, pl.ds(pl.multiple_of(at, SUB), SUB), :] = i
            chance[at // strip, b, pl.ds(pl.multiple_of(at % strip, SUB), SUB), :] = r * r + i * i
        return 0

    lax.fori_loop(0, devices, finish, 0)

    copies = []
    for step in range(1, n_bank):
        other = (bank + step) % n_bank
        copies.append(pltpu.make_async_remote_copy(
            src_ref=chance.at[other], dst_ref=chances.at[step - 1],
            send_sem=m_send.at[step - 1], recv_sem=m_recv.at[step - 1],
            device_id=(other, lane), device_id_type=MESH,
        ))
        copies[-1].start()
    for copy in copies:
        copy.wait()
    total = chance[bank]
    for step in range(1, n_bank):
        total = total + chances[step - 1]
    marginal_ref[...] = total * (1.0 / n_bank)

    arrive(e_ref, e_send)
    for chunk in range(chunks):
        arrive(sent1.at[chunk], send1.at[chunk])
        arrive(sent2.at[chunk], send2.at[chunk])


def shards(n_bank, n_lane, amplitudes, energies, angles):
    devices = n_bank * n_lane
    _, blocks, rows, lanes = amplitudes.shape
    group = blocks * rows // devices
    chunks = min(CHUNKS, group // SUB)
    piece = group // chunks
    f32 = jnp.float32
    whole = pl.BlockSpec(memory_space=pltpu.VMEM)
    swapped = pltpu.VMEM((chunks, devices, 2, piece, lanes), f32)
    real = pltpu.VMEM((devices, group, lanes), f32)
    strip = (blocks, rows // n_bank, lanes)
    one, many = pltpu.SemaphoreType.DMA, pltpu.SemaphoreType.DMA((chunks,))
    return pl.pallas_call(
        functools.partial(kernel, n_bank, n_lane, chunks),
        out_shape=(
            jax.ShapeDtypeStruct(amplitudes.shape, f32),
            jax.ShapeDtypeStruct(strip, f32),
        ),
        in_specs=[whole] * 4,
        out_specs=(whole, whole),
        scratch_shapes=[
            pltpu.VMEM((blocks, 2, rows, lanes), f32),
            swapped, swapped, swapped, swapped,
            real, real, real,
            pltpu.VMEM((n_bank, *strip), f32),
            pltpu.VMEM((n_bank - 1, *strip), f32),
            one, one, many, many, many, many,
            pltpu.SemaphoreType.DMA((n_bank - 1,)),
            pltpu.SemaphoreType.DMA((n_bank - 1,)),
        ],
        compiler_params=pltpu.CompilerParams(collective_id=0, has_side_effects=True),
        name="walsh",
    )(amplitudes, energies.reshape(devices, group, lanes), angles, walsh_table())


def solution(mesh):
    sizes = mesh.shape
    return jax.shard_map(
        functools.partial(shards, sizes["bank"], sizes["lane"]),
        mesh=mesh,
        in_specs=(P(None, ("bank", "lane"), None, None), P(("bank", "lane"), None, None), P()),
        out_specs=(P(None, ("bank", "lane"), None, None), P("lane", "bank", None)),
        check_vma=False,
    )
```

```python
import functools

import jax
import jax.numpy as jnp
import numpy as np
from jax import lax
from jax.experimental import pallas as pl
from jax.experimental.pallas import tpu as pltpu
from jax.sharding import PartitionSpec as P

MESH = pl.DeviceIdType.MESH
TABLE = 256
SUB = 8


def walsh_table():
    rank = np.arange(TABLE)
    both = rank[:, None] & rank[None, :]
    parity = sum((both >> place) & 1 for place in range(8)) % 2
    return jnp.asarray(np.where(parity == 1, -1.0, 1.0) / 16.0, jnp.bfloat16)


def cos_sin(turn):
    half = turn * 0.5
    x = half * half
    s = -1.0 / 39916800.0
    for term in (1.0 / 362880.0, -1.0 / 5040.0, 1.0 / 120.0, -1.0 / 6.0, 1.0):
        s = s * x + term
    s = s * half
    c = 1.0 / 479001600.0
    for term in (-1.0 / 3628800.0, 1.0 / 40320.0, -1.0 / 720.0, 1.0 / 24.0, -0.5, 1.0):
        c = c * x + term
    return 1.0 - 2.0 * (s * s), 2.0 * (s * c)


def split(values):
    high = values.astype(jnp.bfloat16)
    return high, (values - high.astype(jnp.float32)).astype(jnp.bfloat16)


def mix(items):
    items, step = list(items), 1
    while step < len(items):
        for low in range(len(items)):
            if not low & step:
                u, v = items[low], items[low + step]
                items[low], items[low + step] = u + v, u - v
        step *= 2
    return items


def dot(a, b):
    return jnp.dot(a, b, preferred_element_type=jnp.float32)


def mix_lanes(values, table):
    high, low = split(values)
    return dot(jnp.concatenate([high, low], axis=1), table[:, :128])


def kernel(
    n_bank, n_lane, chunks,
    a_hbm, e_hbm, angle_hbm, table_hbm,
    out_ref, marginal_ref,
    a_ref, e_ref, angle_ref, table_ref,
    held, sent1, got1, sent2, got2, levels, cosine, sine, chance, chances,
    in_sem, e_send, e_recv, send1, recv1, send2, recv2, m_send, m_recv,
):
    devices = n_bank * n_lane
    _, blocks, rows, lanes = a_ref.shape
    group = blocks * rows // devices
    groups = rows // group
    bank, lane = lax.axis_index("bank"), lax.axis_index("lane")
    me = bank * n_lane + lane

    fetches = [
        pltpu.make_async_copy(src, dst, in_sem.at[i])
        for i, (src, dst) in enumerate([
            (e_hbm, e_ref), (a_hbm, a_ref), (angle_hbm, angle_ref), (table_hbm, table_ref),
        ])
    ]
    for fetch in fetches:
        fetch.start()

    def others(act):
        half = n_lane // 2

        def around(step, first_bank):
            there = lax.rem(lane + half + step, n_lane)
            for turn in range(first_bank, n_bank):
                act(lax.rem(bank + turn, n_bank), there)
            return 0

        lax.fori_loop(0, half, lambda step, _: around(step, 0), 0)
        lax.fori_loop(half + 1, n_lane, lambda step, _: around(step, 0), 0)
        around(half, 1)

    barrier = pltpu.get_barrier_semaphore()

    def greet(to_bank, to_lane):
        pl.semaphore_signal(
            barrier, inc=1, device_id=(to_bank, to_lane), device_id_type=MESH
        )

    others(greet)
    fetches[0].wait()
    pl.semaphore_wait(barrier, devices - 1)

    def swap(src, dst, send_sem, recv_sem):
        def one(to_bank, to_lane):
            pltpu.make_async_remote_copy(
                src_ref=src.at[to_bank * n_lane + to_lane], dst_ref=dst.at[me],
                send_sem=send_sem, recv_sem=recv_sem,
                device_id=(to_bank, to_lane), device_id_type=MESH,
            ).start()

        others(one)

    def arrive(buffer, sem):
        most = buffer.at[pl.ds(0, devices - 1)]
        pltpu.make_async_copy(most, most, sem).wait()

    swap(e_ref, levels, e_send, e_recv)
    levels[me] = e_ref[me]
    for fetch in fetches[1:]:
        fetch.wait()

    table = table_ref[...]

    def block_step(b, _):
        first = b * groups
        level = e_ref[pl.ds(first, groups)].reshape(rows, lanes)
        c, s = cos_sin(level * angle_ref[0:1, :])
        re, im = a_ref[0, b], a_ref[1, b]
        turned = jnp.concatenate([re * c + im * s, im * c - re * s], axis=0)
        along = mix_lanes(turned, table)
        high, low = split(jnp.concatenate([along[:rows], along[rows:]], axis=1))
        mixed = dot(table[:128, :], jnp.concatenate([high, low], axis=0))
        held[b, 0] = mixed[:, :lanes]
        held[b, 1] = mixed[:, lanes:]
        return 0

    lax.fori_loop(0, blocks, block_step, 0)

    for chunk in range(chunks):
        def spread(g, _, chunk=chunk):
            start = pl.multiple_of(g * group + chunk * SUB, SUB)
            for part in range(2):
                mixed = mix([held[b, part, pl.ds(start, SUB), :] for b in range(blocks)])
                for b in range(blocks):
                    sent1[chunk, b * groups + g, part] = mixed[b]
            return 0

        lax.fori_loop(0, groups, spread, 0)
        swap(sent1.at[chunk], got1.at[chunk], send1.at[chunk], recv1.at[chunk])
        got1[chunk, me] = sent1[chunk, me]

    arrive(levels, e_recv)

    def phases(d, _):
        c, s = cos_sin(levels[d] * angle_ref[1:2, :])
        cosine[d] = c
        sine[d] = s
        return 0

    lax.fori_loop(0, devices, phases, 0)

    wide = TABLE // SUB
    lag = 2 if chunks > 1 else 1
    for chunk in range(chunks):
        arrive(got1.at[chunk], recv1.at[chunk])
        there = pl.ds(chunk * SUB, SUB)
        re = mix([got1[chunk, d, 0] for d in range(devices)])
        im = mix([got1[chunk, d, 1] for d in range(devices)])
        done = []
        for start in range(0, devices, wide):
            r, i = [], []
            for d in range(start, start + wide):
                c, s = cosine[d, there, :], sine[d, there, :]
                r.append(re[d] * c + im[d] * s)
                i.append(im[d] * c - re[d] * s)
            along = mix_lanes(jnp.concatenate(r + i, axis=0), table)
            pair = jnp.concatenate([along[:TABLE], along[TABLE:]], axis=1)
            high, low = split(pair)
            done.append(dot(table, high) + dot(table, low))
        done = mix(done)
        for d in range(devices):
            at = d % wide * SUB
            for part in range(2):
                tile = done[d // wide][at : at + SUB, part * lanes : (part + 1) * lanes]
                if chunk % lag:
                    before = sent2[chunk - 1, d, part]
                    sent2[chunk - 1, d, part] = before + tile
                    sent2[chunk, d, part] = before - tile
                else:
                    sent2[chunk, d, part] = tile
        if chunk % lag == lag - 1:
            for ready in range(chunk - lag + 1, chunk + 1):
                swap(sent2.at[ready], got2.at[ready], send2.at[ready], recv2.at[ready])
                got2[ready, me] = sent2[ready, me]

    scale = float(TABLE * TABLE) / (devices * blocks * rows * lanes)
    pieces = lag
    layers = chunks // pieces
    share = rows // n_bank // group

    def back(chunk, part):
        return mix([got2[chunk, d, part] for d in range(devices)])

    for chunk in range(chunks - pieces):
        arrive(got2.at[chunk], recv2.at[chunk])
        for part in range(2):
            mixed = back(chunk, part)
            for d in range(devices):
                got2[chunk, d, part] = mixed[d]

    copies = []
    for piece in range(pieces):
        last = chunks - pieces + piece
        arrive(got2.at[last], recv2.at[last])
        for part in range(2):
            mixed = back(last, part)
            for d in range(devices):
                tiles = [got2[t, d, part] for t in range(piece, last, pieces)]
                tiles = mix(tiles + [mixed[d]])
                b, g = divmod(d, groups)
                for t in range(layers):
                    value = tiles[t] * scale
                    at = g * group + (t * pieces + piece) * SUB
                    out_ref[part, b, at : at + SUB, :] = value
                    spot = (piece, g // share, b, pl.ds((g % share * layers + t) * SUB, SUB))
                    square = value * value
                    chance[spot] = chance[spot] + square if part else square
        for step in range(1, n_bank):
            other = lax.rem(bank + step, n_bank)
            copies.append(pltpu.make_async_remote_copy(
                src_ref=chance.at[piece, other], dst_ref=chances.at[piece, step - 1],
                send_sem=m_send.at[piece, step - 1], recv_sem=m_recv.at[piece, step - 1],
                device_id=(other, lane), device_id_type=MESH,
            ))
            copies[-1].start()
    for piece in range(pieces):
        for copy in copies[piece * (n_bank - 1) : (piece + 1) * (n_bank - 1)]:
            copy.wait_recv()
        total = chance[piece, bank]
        for step in range(1, n_bank):
            total = total + chances[piece, step - 1]
        total = total * (1.0 / n_bank)
        for g in range(share):
            for t in range(layers):
                at = g * group + (t * pieces + piece) * SUB
                of = (g * layers + t) * SUB
                marginal_ref[:, at : at + SUB, :] = total[:, of : of + SUB]

    for copy in copies:
        copy.wait_send()
    arrive(e_ref, e_send)
    for chunk in range(chunks):
        arrive(sent1.at[chunk], send1.at[chunk])
        arrive(sent2.at[chunk], send2.at[chunk])


def shards(n_bank, n_lane, amplitudes, energies, angles):
    devices = n_bank * n_lane
    _, blocks, rows, lanes = amplitudes.shape
    group = blocks * rows // devices
    chunks = group // SUB
    pieces = min(2, chunks)
    f32 = jnp.float32
    table = walsh_table()
    whole = pl.BlockSpec(memory_space=pltpu.VMEM)
    swapped = pltpu.VMEM((chunks, devices, 2, SUB, lanes), f32)
    real = pltpu.VMEM((devices, group, lanes), f32)
    strip = (blocks, rows // n_bank, lanes)
    part = (blocks, rows // n_bank // pieces, lanes)
    one, many = pltpu.SemaphoreType.DMA, pltpu.SemaphoreType.DMA((chunks,))
    return pl.pallas_call(
        functools.partial(kernel, n_bank, n_lane, chunks),
        out_shape=(
            pltpu.VMEM(amplitudes.shape, f32),
            pltpu.VMEM(strip, f32),
        ),
        in_specs=[pl.BlockSpec(memory_space=pltpu.HBM)] * 4,
        out_specs=(whole, whole),
        scratch_shapes=[
            pltpu.VMEM(amplitudes.shape, f32),
            real,
            pltpu.VMEM(angles.shape, f32),
            pltpu.VMEM(table.shape, table.dtype),
            pltpu.VMEM((blocks, 2, rows, lanes), f32),
            swapped, swapped, swapped, swapped,
            real, real, real,
            pltpu.VMEM((pieces, n_bank, *part), f32),
            pltpu.VMEM((pieces, n_bank - 1, *part), f32),
            pltpu.SemaphoreType.DMA((4,)),
            one, one, many, many, many, many,
            pltpu.SemaphoreType.DMA((pieces, n_bank - 1)),
            pltpu.SemaphoreType.DMA((pieces, n_bank - 1)),
        ],
        compiler_params=pltpu.CompilerParams(
            collective_id=0, has_side_effects=True
        ),
        name="walsh",
    )(amplitudes, energies.reshape(devices, group, lanes), angles, table)


def solution(mesh):
    sizes = mesh.shape
    return jax.shard_map(
        functools.partial(shards, sizes["bank"], sizes["lane"]),
        mesh=mesh,
        in_specs=(P(None, ("bank", "lane"), None, None), P(("bank", "lane"), None, None), P()),
        out_specs=(P(None, ("bank", "lane"), None, None), P("lane", "bank", None)),
        check_vma=False,
    )
```

```python
import functools

import jax
import jax.numpy as jnp
import numpy as np
from jax import lax
from jax.experimental import pallas as pl
from jax.experimental.pallas import tpu as pltpu
from jax.sharding import PartitionSpec as P

MESH = pl.DeviceIdType.MESH
TABLE = 256
SUB = 8


def walsh_table():
    rank = np.arange(TABLE)
    both = rank[:, None] & rank[None, :]
    parity = sum((both >> place) & 1 for place in range(8)) % 2
    return jnp.asarray(np.where(parity == 1, -1.0, 1.0) / 16.0, jnp.bfloat16)


def cos_sin(turn):
    half = turn * 0.5
    x = half * half
    s = -1.0 / 39916800.0
    for term in (1.0 / 362880.0, -1.0 / 5040.0, 1.0 / 120.0, -1.0 / 6.0, 1.0):
        s = s * x + term
    s = s * half
    c = 1.0 / 479001600.0
    for term in (-1.0 / 3628800.0, 1.0 / 40320.0, -1.0 / 720.0, 1.0 / 24.0, -0.5, 1.0):
        c = c * x + term
    return 1.0 - 2.0 * (s * s), 2.0 * (s * c)


def split(values):
    high = values.astype(jnp.bfloat16)
    return high, (values - high.astype(jnp.float32)).astype(jnp.bfloat16)


def mix(items):
    items, step = list(items), 1
    while step < len(items):
        for low in range(len(items)):
            if not low & step:
                u, v = items[low], items[low + step]
                items[low], items[low + step] = u + v, u - v
        step *= 2
    return items


def dot(a, b):
    return jnp.dot(a, b, preferred_element_type=jnp.float32)


def mix_lanes(values, table):
    high, low = split(values)
    return dot(jnp.concatenate([high, low], axis=1), table[:, :128])


def kernel(
    n_bank, n_lane, chunks,
    a_hbm, e_hbm, angle_hbm, table_hbm,
    out_ref, marginal_ref,
    a_ref, e_ref, angle_ref, table_ref,
    held, sent1, got1, sent2, got2, levels, cosine, sine, chance, chances,
    in_sem, e_send, e_recv, send1, recv1, send2, recv2, m_send, m_recv,
):
    devices = n_bank * n_lane
    _, blocks, rows, lanes = a_ref.shape
    group = blocks * rows // devices
    groups = rows // group
    bank, lane = lax.axis_index("bank"), lax.axis_index("lane")
    me = bank * n_lane + lane

    fetches = [
        pltpu.make_async_copy(src, dst, in_sem.at[i])
        for i, (src, dst) in enumerate([
            (e_hbm, e_ref), (a_hbm, a_ref), (angle_hbm, angle_ref), (table_hbm, table_ref),
        ])
    ]
    for fetch in fetches:
        fetch.start()

    def others(act):
        half = n_lane // 2

        def around(step, first_bank):
            there = lax.rem(lane + half + step, n_lane)
            for turn in range(first_bank, n_bank):
                act(lax.rem(bank + turn, n_bank), there)
            return 0

        lax.fori_loop(0, half, lambda step, _: around(step, 0), 0)
        lax.fori_loop(half + 1, n_lane, lambda step, _: around(step, 0), 0)
        around(half, 1)

    barrier = pltpu.get_barrier_semaphore()

    def greet(to_bank, to_lane):
        pl.semaphore_signal(
            barrier, inc=1, device_id=(to_bank, to_lane), device_id_type=MESH
        )

    others(greet)
    fetches[0].wait()
    pl.semaphore_wait(barrier, devices - 1)

    def swap(src, dst, send_sem, recv_sem):
        def one(to_bank, to_lane):
            pltpu.make_async_remote_copy(
                src_ref=src.at[to_bank * n_lane + to_lane], dst_ref=dst.at[me],
                send_sem=send_sem, recv_sem=recv_sem,
                device_id=(to_bank, to_lane), device_id_type=MESH,
            ).start()

        others(one)

    def arrive(buffer, sem):
        most = buffer.at[pl.ds(0, devices - 1)]
        pltpu.make_async_copy(most, most, sem).wait()

    swap(e_ref, levels, e_send, e_recv)
    levels[me] = e_ref[me]
    for fetch in fetches[1:]:
        fetch.wait()

    table = table_ref[...]

    def block_step(b, _):
        first = b * groups
        level = e_ref[pl.ds(first, groups)].reshape(rows, lanes)
        c, s = cos_sin(level * angle_ref[0:1, :])
        re, im = a_ref[0, b], a_ref[1, b]
        turned = jnp.concatenate([re * c + im * s, im * c - re * s], axis=0)
        along = mix_lanes(turned, table)
        high, low = split(jnp.concatenate([along[:rows], along[rows:]], axis=1))
        mixed = dot(table[:128, :], jnp.concatenate([high, low], axis=0))
        held[b, 0] = mixed[:, :lanes]
        held[b, 1] = mixed[:, lanes:]
        return 0

    lax.fori_loop(0, blocks, block_step, 0)

    for chunk in range(chunks):
        def spread(g, _, chunk=chunk):
            start = pl.multiple_of(g * group + chunk * SUB, SUB)
            for part in range(2):
                mixed = mix([held[b, part, pl.ds(start, SUB), :] for b in range(blocks)])
                for b in range(blocks):
                    sent1[chunk, b * groups + g, part] = mixed[b]
            return 0

        lax.fori_loop(0, groups, spread, 0)
        swap(sent1.at[chunk], got1.at[chunk], send1.at[chunk], recv1.at[chunk])
        got1[chunk, me] = sent1[chunk, me]

    arrive(levels, e_recv)

    def phases(d, _):
        c, s = cos_sin(levels[d] * angle_ref[1:2, :])
        cosine[d] = c
        sine[d] = s
        return 0

    lax.fori_loop(0, devices, phases, 0)

    wide = TABLE // SUB
    lag = 2 if chunks > 1 else 1
    for chunk in range(chunks):
        arrive(got1.at[chunk], recv1.at[chunk])
        there = pl.ds(chunk * SUB, SUB)
        re = mix([got1[chunk, d, 0] for d in range(devices)])
        im = mix([got1[chunk, d, 1] for d in range(devices)])
        done = []
        for start in range(0, devices, wide):
            r, i = [], []
            for d in range(start, start + wide):
                c, s = cosine[d, there, :], sine[d, there, :]
                r.append(re[d] * c + im[d] * s)
                i.append(im[d] * c - re[d] * s)
            along = mix_lanes(jnp.concatenate(r + i, axis=0), table)
            pair = jnp.concatenate([along[:TABLE], along[TABLE:]], axis=1)
            high, low = split(pair)
            done.append(dot(table, high) + dot(table, low))
        done = mix(done)
        for d in range(devices):
            at = d % wide * SUB
            for part in range(2):
                tile = done[d // wide][at : at + SUB, part * lanes : (part + 1) * lanes]
                if chunk % lag:
                    before = sent2[chunk - 1, d, part]
                    sent2[chunk - 1, d, part] = before + tile
                    sent2[chunk, d, part] = before - tile
                else:
                    sent2[chunk, d, part] = tile
        if chunk % lag == lag - 1:
            for ready in range(chunk - lag + 1, chunk + 1):
                swap(sent2.at[ready], got2.at[ready], send2.at[ready], recv2.at[ready])
                got2[ready, me] = sent2[ready, me]

    scale = float(TABLE * TABLE) / (devices * blocks * rows * lanes)
    pieces = lag
    layers = chunks // pieces
    share = rows // n_bank // group

    def back(chunk, part):
        return mix([got2[chunk, d, part] for d in range(devices)])

    for chunk in range(chunks - pieces):
        arrive(got2.at[chunk], recv2.at[chunk])
        for part in range(2):
            mixed = back(chunk, part)
            for d in range(devices):
                got2[chunk, d, part] = mixed[d]

    copies = []
    for piece in range(pieces):
        last = chunks - pieces + piece
        arrive(got2.at[last], recv2.at[last])
        for part in range(2):
            mixed = back(last, part)
            for d in range(devices):
                tiles = [got2[t, d, part] for t in range(piece, last, pieces)]
                tiles = mix(tiles + [mixed[d]])
                b, g = divmod(d, groups)
                for t in range(layers):
                    value = tiles[t] * scale
                    at = g * group + (t * pieces + piece) * SUB
                    out_ref[part, b, at : at + SUB, :] = value
                    spot = (piece, g // share, b, pl.ds((g % share * layers + t) * SUB, SUB))
                    square = value * value
                    chance[spot] = chance[spot] + square if part else square
        for step in range(1, n_bank):
            other = lax.rem(bank + step, n_bank)
            copies.append(pltpu.make_async_remote_copy(
                src_ref=chance.at[piece, other], dst_ref=chances.at[piece, step - 1],
                send_sem=m_send.at[piece, step - 1], recv_sem=m_recv.at[piece, step - 1],
                device_id=(other, lane), device_id_type=MESH,
            ))
            copies[-1].start()
    for piece in range(pieces):
        for copy in copies[piece * (n_bank - 1) : (piece + 1) * (n_bank - 1)]:
            copy.wait_recv()
        total = chance[piece, bank]
        for step in range(1, n_bank):
            total = total + chances[piece, step - 1]
        total = total * (1.0 / n_bank)
        for g in range(share):
            for t in range(layers):
                at = g * group + (t * pieces + piece) * SUB
                of = (g * layers + t) * SUB
                marginal_ref[:, at : at + SUB, :] = total[:, of : of + SUB]

    for copy in copies:
        copy.wait_send()
    arrive(e_ref, e_send)
    for chunk in range(chunks):
        arrive(sent1.at[chunk], send1.at[chunk])
        arrive(sent2.at[chunk], send2.at[chunk])


def put_out(state_ref, marginal_ref, state_out, marginal_out, sem):
    copies = [
        pltpu.make_async_copy(state_ref, state_out, sem.at[0]),
        pltpu.make_async_copy(marginal_ref, marginal_out, sem.at[1]),
    ]
    for copy in copies:
        copy.start()
    for copy in copies:
        copy.wait()


def shards(n_bank, n_lane, amplitudes, energies, angles):
    devices = n_bank * n_lane
    _, blocks, rows, lanes = amplitudes.shape
    group = blocks * rows // devices
    chunks = group // SUB
    pieces = min(2, chunks)
    f32 = jnp.float32
    table = walsh_table()
    whole = pl.BlockSpec(memory_space=pltpu.VMEM)
    swapped = pltpu.VMEM((chunks, devices, 2, SUB, lanes), f32)
    real = pltpu.VMEM((devices, group, lanes), f32)
    strip = (blocks, rows // n_bank, lanes)
    part = (blocks, rows // n_bank // pieces, lanes)
    one, many = pltpu.SemaphoreType.DMA, pltpu.SemaphoreType.DMA((chunks,))
    state, marginal = pl.pallas_call(
        functools.partial(kernel, n_bank, n_lane, chunks),
        out_shape=(
            pltpu.VMEM(amplitudes.shape, f32),
            pltpu.VMEM(strip, f32),
        ),
        in_specs=[pl.BlockSpec(memory_space=pltpu.HBM)] * 4,
        out_specs=(whole, whole),
        scratch_shapes=[
            pltpu.VMEM(amplitudes.shape, f32),
            real,
            pltpu.VMEM(angles.shape, f32),
            pltpu.VMEM(table.shape, table.dtype),
            pltpu.VMEM((blocks, 2, rows, lanes), f32),
            swapped, swapped, swapped, swapped,
            real, real, real,
            pltpu.VMEM((pieces, n_bank, *part), f32),
            pltpu.VMEM((pieces, n_bank - 1, *part), f32),
            pltpu.SemaphoreType.DMA((4,)),
            one, one, many, many, many, many,
            pltpu.SemaphoreType.DMA((pieces, n_bank - 1)),
            pltpu.SemaphoreType.DMA((pieces, n_bank - 1)),
        ],
        compiler_params=pltpu.CompilerParams(
            collective_id=0, has_side_effects=True
        ),
        name="walsh",
    )(amplitudes, energies.reshape(devices, group, lanes), angles, table)
    return pl.pallas_call(
        put_out,
        out_shape=(
            jax.ShapeDtypeStruct(state.shape, f32),
            jax.ShapeDtypeStruct(marginal.shape, f32),
        ),
        in_specs=[whole] * 2,
        out_specs=(pl.BlockSpec(memory_space=pltpu.HBM),) * 2,
        scratch_shapes=[pltpu.SemaphoreType.DMA((2,))],
        compiler_params=pltpu.CompilerParams(vmem_limit_bytes=1024 * 1024),
        name="put_out",
    )(state, marginal)


def solution(mesh):
    sizes = mesh.shape
    return jax.shard_map(
        functools.partial(shards, sizes["bank"], sizes["lane"]),
        mesh=mesh,
        in_specs=(P(None, ("bank", "lane"), None, None), P(("bank", "lane"), None, None), P()),
        out_specs=(P(None, ("bank", "lane"), None, None), P("lane", "bank", None)),
        check_vma=False,
    )
```
